256 devices in a mesh: parts: 2 (over y), dp: 64 (over x, z), tensor: 2 (over core).
Axes of the slice: x: 4, y: 2, z: 16, core: 2. Of those that a mesh axis runs over, the one named last changes fastest.
The devices are a block of a 4x16x16 slice.
Arguments:
- normed: bfloat16 [128, 256, 4096], P(('parts', 'dp')), parts along dimension 0, may hold values from -28 to 28
- q_weight: bfloat16 [4096, 2048], P('dp', 'tensor'), may hold values from -0.09375 to 0.09375
- kv_weight: bfloat16 [4096, 2, 512], P('dp', None, 'tensor'), may hold values from -0.09375 to 0.09375
- o_weight: bfloat16 [2048, 4096], P('tensor', 'dp'), may hold values from -0.5 to 0.5
- lengths: int32 [128], P(('parts', 'dp')), parts along dimension 0, may hold values from 64 to 256
- destinations: int32 [128], P(('parts', 'dp')), parts along dimension 0, may hold values from 0 to 63, each once
Outputs:
- projected: bfloat16 [128, 256, 4096], P(('parts', 'dp'), None, 'tensor'), parts along dimension 0
- kv_cache: bfloat16 [128, 2, 4, 256, 128], P(('parts', 'dp'), None, None, 'tensor'), parts along dimension 0
The draws below stay inside these ranges and needn't reach their ends.
There are 2 independent parts, one for each index of `parts`. The reference program is written for one: setup_inputs(seed, part) draws one part's arguments, and reference() takes and returns one part's arrays. A program takes and returns all parts, laid end to end along the dimension named above; an argument that names none is the same for every part. Nothing has to cross between parts.
All inputs are finite; a program needn't handle non-finite values.
Results may differ from the reference program's by a relative error of at most 0.012.
The reference program's roundings to bfloat16 on the way (of `query`, `keys`, `weights`, `attended` and `cache`) count: a program that leaves them out, or rounds other values in their place, can miss the bound.
Values may be sent and summed in bfloat16 or wider, within the bound.
No kernel may reach another device: no remote copies, remote signals or barrier semaphores. Data moves between devices by JAX's collectives and lax.ppermute only.
A program may use at most 128 MiB of HBM per device.

```python
import math
import jax
import jax.numpy as jnp
from jax import lax

D = 4096
HD = 128
HEADS = 16
KV_HEADS = 4
LEN = 256
PROMPTS = 64


def draw_normed(key, part):
    shape = (PROMPTS, LEN, D)
    base_key = jax.random.fold_in(key, 11)
    values = jax.random.truncated_normal(base_key, -6.0, 6.0, shape, jnp.float32)
    return values.astype(jnp.bfloat16)


def touch_ends(drawn, stream_key, low, high):
    dims = drawn.shape
    place = [jax.random.randint(jax.random.fold_in(stream_key, axis), (), 0, dims[axis]) for axis in range(len(dims))]
    drawn = drawn.at[tuple(place)].set(low)
    longest = dims.index(max(dims))
    place[longest] = (place[longest] + 1) % dims[longest]
    return drawn.at[tuple(place)].set(high)


def level_of(key, extent, split, smallest, top_value):
    factor_of = 1.0
    for dim, blocks in split:
        draws = jax.random.uniform(jax.random.fold_in(jax.random.fold_in(key, 6), dim), (blocks,), jnp.float32, smallest / len(split), top_value / len(split))
        factor_of = factor_of * jnp.repeat(jnp.exp(draws), extent[dim] // blocks).reshape((-1,) + (1,) * (len(extent) - 1 - dim))
    return factor_of


def scatter_about(stream_key, shape, deviation, bound, shards=(), kind=jnp.bfloat16):
    loudness = level_of(stream_key, shape, shards, -0.22, 0.18) if shards else 1.0
    result = jax.random.normal(stream_key, shape, jnp.float32) * deviation * loudness
    return jnp.minimum(jnp.maximum(result, -bound), bound).astype(kind)


def setup_inputs(seed: int = 0, part: int = 0) -> dict:
    key_list = jax.random.split(jax.random.key(seed), 7)
    part_splits = jax.random.split(jax.random.fold_in(key_list[6], part), 7)
    normed = draw_normed(jax.random.fold_in(jax.random.fold_in(key_list[6], part), 71), part)
    q_weight = scatter_about(key_list[1], (D, HEADS * HD), D ** -0.5, 0.09375, ((0, 64), (1, 2)))
    kv_weight = scatter_about(key_list[2], (D, 2, KV_HEADS * HD), D ** -0.5, 0.09375, ((0, 64), (2, 2)))
    o_weight = scatter_about(key_list[3], (HEADS * HD, D), HD ** -0.5, 0.5, ((0, 2), (1, 64)))
    lengths = touch_ends(jax.random.randint(part_splits[4], (PROMPTS,), LEN // 4, LEN + 1), jax.random.fold_in(part_splits[4], 1), LEN // 4, LEN).astype(jnp.int32)
    destinations = jax.random.permutation(part_splits[5], PROMPTS).astype(jnp.int32)
    return dict(normed=normed, q_weight=q_weight, kv_weight=kv_weight, o_weight=o_weight, lengths=lengths, destinations=destinations)


ROPE_BASE = 500000.0

def rotate(values, positions):
    half = values.shape[-1] // 2
    steps = jnp.arange(half, dtype=jnp.float32) * (2.0 / values.shape[-1])
    freq = jnp.power(jnp.float32(ROPE_BASE), -steps)
    angle = positions.astype(jnp.float32)[:, None] * freq[None, :]
    cosine = jnp.cos(angle)[:, None, :]
    sine = jnp.sin(angle)[:, None, :]
    first = values[..., :half]
    second = values[..., half:]
    return jnp.concatenate([first * cosine - second * sine, second * cosine + first * sine], axis=-1)

def reference(normed, q_weight, kv_weight, o_weight, lengths, destinations):

    def one_prompt(item):
        tokens, length = item
        total = tokens.shape[0]
        positions = jnp.arange(total, dtype=jnp.int32)
        query = jnp.dot(tokens, q_weight, preferred_element_type=jnp.float32).reshape(total, HEADS, HD)
        query = rotate(query, positions).astype(jnp.bfloat16)
        pair = jnp.dot(tokens, kv_weight.reshape(D, 2 * KV_HEADS * HD), preferred_element_type=jnp.float32)
        pair = pair.reshape(total, 2, KV_HEADS, HD)
        keys = rotate(pair[:, 0], positions).astype(jnp.bfloat16)
        values = pair[:, 1].astype(jnp.bfloat16)
        group = HEADS // KV_HEADS
        grouped = query.reshape(total, KV_HEADS, group, HD).transpose(1, 2, 0, 3).astype(jnp.float32)
        key_rows = keys.transpose(1, 0, 2).astype(jnp.float32)
        value_rows = values.transpose(1, 0, 2).astype(jnp.float32)
        scores = jnp.einsum('kgqd,ktd->kgqt', grouped, key_rows, precision=lax.Precision.HIGHEST) / math.sqrt(HD)
        allowed = (positions[:, None] >= positions[None, :]) & (positions[None, :] < length)
        scores = jnp.where(allowed, scores, -jnp.inf)
        peak = lax.optimization_barrier(jnp.max(scores, axis=-1, keepdims=True))
        expo = jnp.exp(scores - peak)
        weights = (expo / lax.optimization_barrier(jnp.sum(expo, axis=-1, keepdims=True))).astype(jnp.bfloat16)
        attended = jnp.einsum('kgqt,ktd->kgqd', weights.astype(jnp.float32), value_rows, precision=lax.Precision.HIGHEST)
        attended = attended.astype(jnp.bfloat16).transpose(2, 0, 1, 3).reshape(total, HEADS * HD)
        projected = jnp.dot(attended, o_weight, preferred_element_type=jnp.float32).astype(jnp.bfloat16)
        live = (positions < length)[:, None, None]
        kept_keys = jnp.where(live, keys, jnp.zeros_like(keys))
        kept_values = jnp.where(live, values, jnp.zeros_like(values))
        cache = jnp.stack([kept_keys, kept_values], axis=0).transpose(0, 2, 1, 3)
        return (projected, cache)
    projected, caches = lax.map(one_prompt, (normed, lengths))
    slots = jnp.arange(PROMPTS, dtype=jnp.int32)
    match = destinations[None, :] == slots[:, None]
    source = lax.optimization_barrier(jnp.sum(jnp.where(match, slots[None, :], 0), axis=1)).astype(jnp.int32)
    return (projected, jnp.take(caches, source, axis=0))
```

```python
import functools
import math

import jax
import jax.numpy as jnp
import numpy as np
from jax import lax
from jax.experimental import pallas as pl
from jax.experimental.pallas import tpu as pltpu
from jax.sharding import PartitionSpec as P

HD = 128
ROPE_BASE = 500000.0
X = 4


def mover(ring):
    def move(array, where):
        pairs = []
        for x in range(X):
            for z in range(ring):
                for t in range(2):
                    a, b, c = where(x, z, t)
                    target = ((a % X) * ring + b % ring) * 2 + c
                    pairs.append(((x * ring + z) * 2 + t, target))
        return lax.ppermute(array, ("dp", "tensor"), pairs)

    return move


def project_kernel(pair_ref, x_ref, w_ref, out_ref):
    slots, total, depth = x_ref.shape
    weights = w_ref[...].reshape(depth, w_ref.shape[2])
    product = jnp.dot(
        x_ref[...].reshape(slots * total, depth), weights, preferred_element_type=jnp.float32
    ).reshape(slots, total, -1)
    width = weights.shape[1]
    columns = pl.ds(pl.multiple_of(pl.program_id(1) * width, width), width)

    @pl.when(pl.program_id(0) == 0)
    def _():
        out_ref[:, :, columns] = product

    @pl.when(pl.program_id(0) > 0)
    def _():
        out_ref[:, :, columns] += product


def project_in(states, weights, pair, pieces=3):
    _, total, half = states.shape
    ring, rows, both = weights.shape
    wide = both // 2
    return pl.pallas_call(
        project_kernel,
        grid_spec=pltpu.PrefetchScalarGridSpec(
            num_scalar_prefetch=1,
            grid=(2, pieces),
            in_specs=[
                pl.BlockSpec((2, total, half // 2), lambda b, n, p: (p[0], 0, b)),
                pl.BlockSpec((ring, rows, wide // pieces), lambda b, n, p: (0, 0, b * pieces + n)),
            ],
            out_specs=pl.BlockSpec((2, total, wide), lambda b, n, p: (0, 0, 0)),
        ),
        out_shape=jax.ShapeDtypeStruct((2, total, wide), jnp.float32),
        compiler_params=pltpu.CompilerParams(vmem_limit_bytes=24 << 20),
        name="project_in",
    )(pair.reshape(1), states, weights)


def attend_kernel(heads, a_ref, b_ref, l0_ref, l1_ref, turn_ref, out_ref, cache_ref):
    note = jnp.where(pl.program_id(0) == 0, l0_ref[:1, :1], l1_ref[:1, :1])
    length = note.astype(jnp.float32).astype(jnp.int32)
    cosine = jnp.concatenate([turn_ref[:, : HD // 2]] * 2, axis=1)
    sine = jnp.concatenate([-turn_ref[:, HD // 2 :], turn_ref[:, HD // 2 :]], axis=1)
    total = a_ref.shape[1]

    def part(index):
        columns = slice(index * HD, (index + 1) * HD)
        return a_ref[0, :, columns] + b_ref[0, :, columns]

    def turned(values):
        swapped = pltpu.roll(values, HD // 2, 1)
        return (values * cosine + swapped * sine).astype(jnp.bfloat16)

    keys = turned(part(heads))
    values = part(heads + 1).astype(jnp.bfloat16)
    live = lax.broadcasted_iota(jnp.int32, (total, HD), 0) < length
    zero = jnp.zeros((), jnp.bfloat16)
    cache_ref[0, 0] = jnp.where(live, keys, zero)
    cache_ref[0, 1] = jnp.where(live, values, zero)
    row = lax.broadcasted_iota(jnp.int32, (total, total), 0)
    column = lax.broadcasted_iota(jnp.int32, (total, total), 1)
    allowed = (row >= column) & (column < length)
    for h in range(heads):
        scores = lax.dot_general(
            turned(part(h)), keys, (((1,), (1,)), ((), ())), preferred_element_type=jnp.float32
        ) * (1.0 / math.sqrt(HD))
        scores = jnp.where(allowed, scores, -jnp.inf)
        peak = jnp.max(scores, axis=-1, keepdims=True)
        expo = jnp.exp(scores - peak)
        share = 1.0 / jnp.sum(expo, axis=-1, keepdims=True)
        weights = (expo * share).astype(jnp.bfloat16)
        out_ref[:, h * HD : (h + 1) * HD] = jnp.dot(
            weights, values, preferred_element_type=jnp.float32
        ).astype(jnp.bfloat16)


def turns(total):
    steps = np.arange(HD // 2, dtype=np.float32) * np.float32(2.0 / HD)
    freq = np.power(np.float32(ROPE_BASE), -steps)
    angle = np.arange(total, dtype=np.float32)[:, None] * freq[None, :]
    return np.concatenate([np.cos(angle), np.sin(angle)], axis=1).astype(np.float32)


def attend(kept, other, first, second, heads):
    _, total, wide = kept.shape
    rows = pl.BlockSpec((1, total, wide), lambda s: (s, 0, 0))
    note = pl.BlockSpec((16, HD), lambda s: (0, wide // HD))
    return pl.pallas_call(
        functools.partial(attend_kernel, heads),
        grid=(2,),
        in_specs=[rows, rows, note, note, pl.BlockSpec((total, HD), lambda s: (0, 0))],
        out_specs=[
            pl.BlockSpec((total, heads * HD), lambda s: (s, 0)),
            pl.BlockSpec((1, 2, total, HD), lambda s: (s, 0, 0, 0)),
        ],
        out_shape=[
            jax.ShapeDtypeStruct((2 * total, heads * HD), jnp.bfloat16),
            jax.ShapeDtypeStruct((2, 2, total, HD), jnp.bfloat16),
        ],
        compiler_params=pltpu.CompilerParams(vmem_limit_bytes=24 << 20),
        name="attend",
    )(kept, other, first, second, turns(total))


def output_kernel(shift_ref, a0, a1, a2, a3, a4, near_ref, far_ref, out_ref, line_ref):
    half = a0.shape[0] // 2

    @pl.when(pl.program_id(0) == 0)
    def _():
        for d, start, rows in ((0, 0, a0), (1, 0, a1), (2, 0, a2), (2, half, a3), (3, 0, a4)):
            place = (d + shift_ref[0]) % X
            line_ref[place, start : start + rows.shape[0], :] = rows[...]

    group = a0.shape[1]
    total = 0.0
    for place in range(X):
        ref = near_ref if place < X // 2 else far_ref
        start = place % (X // 2) * group
        total += lax.dot_general(
            line_ref[place],
            ref[:, start : start + group],
            (((1,), (1,)), ((), ())),
            preferred_element_type=jnp.float32,
        )
    out_ref[...] = total.astype(out_ref.dtype)


def project_out(mine, after, across, before, near, far, shift, pieces=4):
    total, group = mine.shape
    columns = near.shape[0]
    whole = pl.BlockSpec((total, group), lambda i, w: (0, 0))
    part = pl.BlockSpec((total // 2, group), lambda i, w: (0, 0))
    weights = pl.BlockSpec((columns // pieces, near.shape[1]), lambda i, w: (i, 0))
    return pl.pallas_call(
        output_kernel,
        grid_spec=pltpu.PrefetchScalarGridSpec(
            num_scalar_prefetch=1,
            grid=(pieces,),
            in_specs=[whole, whole, part, part, whole, weights, weights],
            out_specs=pl.BlockSpec((total, columns // pieces), lambda i, w: (0, i)),
            scratch_shapes=[pltpu.VMEM((X, total, group), mine.dtype)],
        ),
        out_shape=jax.ShapeDtypeStruct((total, columns), jnp.bfloat16),
        compiler_params=pltpu.CompilerParams(vmem_limit_bytes=24 << 20),
        name="project_out",
    )(shift.reshape(1), mine, after, *across, before, near, far)


def on_device(normed, q_weight, kv_weight, o_weight, lengths, destinations):
    count = lax.axis_size("dp")
    ring = count // X
    move = mover(ring)
    spot = lax.axis_index("dp")
    x, z, t = spot // ring, spot % ring, lax.axis_index("tensor")
    odd = x % 2 == 1

    total, width = normed.shape[1:]
    rows = q_weight.shape[0]
    group = q_weight.shape[1] // 2
    heads = group // HD
    plus = lambda x, z, t: (x + 1, z, t)
    minus = lambda x, z, t: (x - 1, z, t)
    up = lambda x, z, t: (x, z + 1, t)
    down = lambda x, z, t: (x, z - 1, t)
    swap = lambda x, z, t: (x, z, 1 - t)

    note = jnp.broadcast_to(lengths.astype(jnp.bfloat16), (rows, HD))

    def columns(b):
        q = lax.dynamic_slice(q_weight, (0, b * group), (rows, group))
        kv = lax.dynamic_slice(kv_weight, (0, 0, b * HD), (rows, 2, HD))
        return jnp.concatenate([q, kv[:, 0], kv[:, 1], note], axis=1)

    part0 = move(columns(x % 2), lambda x, z, t: (2 * t + x % 2, z, x // 2))
    part1 = move(columns((x + 1) % 2), lambda x, z, t: (2 * t + (x + 1) % 2, z, x // 2))
    first = jnp.where(odd, part1, part0)
    second = jnp.where(odd, part0, part1)
    wide = group + 2 * HD

    block = jnp.concatenate([first[:, :wide], second[:, :wide], o_weight.T], axis=1)
    full_in = jnp.zeros((ring, rows, 2 * wide), block.dtype)
    full_out = jnp.zeros((ring, rows, block.shape[1] - 2 * wide), block.dtype)

    def place(full, block, index, row=0):
        at = (index % ring, row, 0)
        return (
            lax.dynamic_update_slice(full[0], block[None, :, : 2 * wide], at),
            lax.dynamic_update_slice(full[1], block[None, :, 2 * wide :], at),
        )

    full = full_in, full_out
    rising = falling = block
    last = ring // 2
    for k in range(1, last):
        placed = place(full, rising, z - k + 1)
        if k > 1:
            placed = place(placed, falling, z + k - 1)
        rising = move(rising, up)
        falling = move(falling, down)
        rising, falling, full = lax.optimization_barrier((rising, falling, placed))
        if k == 1:
            half = width // 2
            rising, normed = lax.optimization_barrier((rising, normed))
            own = lax.dynamic_slice(normed[0], (0, t * half), (total, half))
            before = move(own, plus)
            after = move(own, minus)
            across0 = move(before[: total // 2], plus)
            across1 = move(after[total // 2 :], minus)
    full = place(place(full, rising, z - last + 1), falling, z + last - 1)
    cut = rows // 2
    full = place(full, move(rising[:cut], up), z - last)
    full_in, full_out = place(full, move(falling[cut:], down), z + last, cut)

    o_half = full_out.reshape(ring * rows, -1)
    o_other = move(o_half, swap)

    states = jnp.zeros((X, total, half), own.dtype)
    for piece, d, row in (
        (own, 0, 0),
        (before, -1, 0),
        (after, 1, 0),
        (across0, 2, 0),
        (across1, 2, total // 2),
    ):
        states = lax.dynamic_update_slice(states, piece[None], ((x + d) % X, row, 0))
    other = move(project_in(states, full_in, 1 - t), swap)
    kept = project_in(states, full_in, t)

    mixed, cache = attend(kept, other, first, second, heads)
    from_before = move(mixed, plus)
    from_after = move(mixed, minus)
    across = move(from_before[:total], plus), move(from_after[total:], minus)
    out = project_out(
        mixed, from_after, across, from_before, o_half, o_other, (x - 2 * t) % X
    )
    out0 = lax.dynamic_slice(out, (x % 2 * total, 0), (total, out.shape[1]))
    out1 = lax.dynamic_slice(out, ((x + 1) % 2 * total, 0), (total, out.shape[1]))
    home0 = move(out0, lambda x, z, t: (2 * t + x % 2, z, x // 2))
    home1 = move(out1, lambda x, z, t: (2 * t + (x + 1) % 2, z, x // 2))
    projected = jnp.concatenate(
        [jnp.where(odd, home1, home0), jnp.where(odd, home0, home1)], axis=1
    )

    cache = cache.reshape(2, 2, 2, total // 2, HD)
    mine = lax.dynamic_index_in_dim(cache, t, 2, keepdims=False)
    theirs = move(lax.dynamic_index_in_dim(cache, 1 - t, 2, keepdims=False), swap)
    four = jnp.concatenate([mine, theirs], axis=0)
    flat = four.reshape(X, count, -1).transpose(1, 0, 2)
    label = jnp.broadcast_to(destinations.astype(jnp.bfloat16), (count, 1, flat.shape[2]))
    spread = lax.all_to_all(
        jnp.concatenate([flat, label], axis=1), "dp", 0, 0, tiled=True
    )
    sent_to = spread[:, X, 0].astype(jnp.int32)
    slots = jnp.arange(count, dtype=jnp.int32)
    match = sent_to[None, :] == slots[:, None]
    source = jnp.sum(jnp.where(match, slots[None, :], 0), axis=1)
    head = jnp.arange(X, dtype=jnp.int32)[None]
    index = (head * ring + (source % ring)[:, None]) * (X + 1)
    index = index + ((source // ring)[:, None] ^ (2 * t))
    outgoing = jnp.take(spread.reshape(count * (X + 1), -1), index.reshape(-1), axis=0)
    arrived = lax.all_to_all(
        outgoing.reshape(count, X, -1), "dp", split_axis=0, concat_axis=0, tiled=True
    )
    routed = arrived.transpose(1, 0, 2).reshape(X, 2, total // 2, HD).transpose(1, 0, 2, 3)
    return (projected[None], routed[None])


def solution(mesh):
    placed = (
        P(("parts", "dp"), None, None),
        P("dp", "tensor"),
        P("dp", None, "tensor"),
        P("tensor", "dp"),
        P(("parts", "dp")),
        P(("parts", "dp")),
    )

    return jax.shard_map(
        on_device,
        mesh=mesh,
        in_specs=placed,
        out_specs=(
            P(("parts", "dp"), None, "tensor"),
            P(("parts", "dp"), None, None, "tensor", None),
        ),
        check_vma=False,
    )
```

```python
import functools
import math

import jax
import jax.numpy as jnp
import numpy as np
from jax import lax
from jax.experimental import pallas as pl
from jax.experimental.pallas import tpu as pltpu
from jax.sharding import Mesh
from jax.sharding import PartitionSpec as P

HD = 128
ROPE_BASE = 500000.0
START = 2
X = 4


def mover(ring):
    def move(array, where):
        pairs = []
        for x in range(X):
            for z in range(ring):
                for t in range(2):
                    a, b, c = where(x, z, t)
                    target = ((a % X) * ring + b % ring) * 2 + c
                    pairs.append(((x * ring + z) * 2 + t, target))
        return lax.ppermute(array, ("x", "z", "tensor"), pairs)

    return move


def project_kernel(pair_ref, x_ref, w_ref, out_ref):
    slots, total, depth = x_ref.shape
    weights = w_ref[...].reshape(depth, w_ref.shape[2])
    product = jnp.dot(
        x_ref[...].reshape(slots * total, depth), weights, preferred_element_type=jnp.float32
    ).reshape(slots, total, -1)
    width = weights.shape[1]
    columns = pl.ds(pl.multiple_of(pl.program_id(1) * width, width), width)

    @pl.when(pl.program_id(0) == 0)
    def _():
        out_ref[:, :, columns] = product

    @pl.when(pl.program_id(0) > 0)
    def _():
        out_ref[:, :, columns] += product


def project_in(states, weights, pair, first, pieces):
    _, total, half = states.shape
    ring, rows, both = weights.shape
    width = 2 * HD
    jump = both // 2 // width
    return pl.pallas_call(
        project_kernel,
        grid_spec=pltpu.PrefetchScalarGridSpec(
            num_scalar_prefetch=1,
            grid=(2, pieces),
            in_specs=[
                pl.BlockSpec((2, total, half // 2), lambda b, n, p: (p[0], 0, b)),
                pl.BlockSpec((ring, rows, width), lambda b, n, p: (0, 0, b * jump + first + n)),
            ],
            out_specs=pl.BlockSpec((2, total, pieces * width), lambda b, n, p: (0, 0, 0)),
        ),
        out_shape=jax.ShapeDtypeStruct((2, total, pieces * width), jnp.float32),
        compiler_params=pltpu.CompilerParams(vmem_limit_bytes=24 << 20),
        name="project_in",
    )(pair.reshape(1), states, weights)


def turned(values, turn_ref):
    cosine = jnp.concatenate([turn_ref[:, : HD // 2]] * 2, axis=1)
    sine = jnp.concatenate([-turn_ref[:, HD // 2 :], turn_ref[:, HD // 2 :]], axis=1)
    swapped = pltpu.roll(values, HD // 2, 1)
    return (values * cosine + swapped * sine).astype(jnp.bfloat16)


def length_of(slot, first_ref, second_ref):
    note = jnp.where(slot == 0, first_ref[:1, :1], second_ref[:1, :1])
    return note.astype(jnp.float32).astype(jnp.int32)


def cache_kernel(a_ref, b_ref, n0_ref, n1_ref, turn_ref, keys_ref, values_ref, sent_ref):
    slot = pl.program_id(0)
    length = length_of(slot, n0_ref, n1_ref)
    total = a_ref.shape[1]
    sums = a_ref[0] + b_ref[0]
    keys = turned(sums[:, :HD], turn_ref)
    values = sums[:, HD:].astype(jnp.bfloat16)
    keys_ref[0] = keys
    values_ref[0] = values
    live = lax.broadcasted_iota(jnp.int32, (total, HD), 0) < length
    zero = jnp.zeros((), jnp.bfloat16)
    ring, cores, _, piece, _ = sent_ref.shape
    count = ring // 2
    for index, array in enumerate((keys, values)):
        kept = jnp.where(live, array, zero).reshape(cores, count, piece, HD)
        for core in range(cores):
            sent_ref[index * count : (index + 1) * count, core, slot] = kept[core]

    @pl.when(slot == 0)
    def _():
        lane = lax.broadcasted_iota(jnp.int32, (piece, HD), 1)
        half = HD // 2
        label = jnp.where(lane == 0, n0_ref[:1, half : half + 1], n1_ref[:1, half : half + 1])
        sent_ref[:, :, 2] = jnp.broadcast_to(label, (ring, cores, piece, HD))


def make_cache(kept, other, first, second, ring):
    _, total, wide = kept.shape
    rows = pl.BlockSpec((1, total, wide), lambda s: (s, 0, 0))
    note = pl.BlockSpec((16, HD), lambda s: (0, first.shape[1] // HD - 1))
    each = pl.BlockSpec((1, total, HD), lambda s: (s, 0, 0))
    sent = (ring, 2, 3, 2 * total // 2 // ring, HD)
    return pl.pallas_call(
        cache_kernel,
        grid=(2,),
        in_specs=[rows, rows, note, note, pl.BlockSpec((total, HD), lambda s: (0, 0))],
        out_specs=[each, each, pl.BlockSpec(sent, lambda s: (0, 0, 0, 0, 0))],
        out_shape=[
            jax.ShapeDtypeStruct((2, total, HD), jnp.bfloat16),
            jax.ShapeDtypeStruct((2, total, HD), jnp.bfloat16),
            jax.ShapeDtypeStruct(sent, jnp.bfloat16),
        ],
        compiler_params=pltpu.CompilerParams(vmem_limit_bytes=24 << 20),
        name="make_cache",
    )(kept, other, first, second, turns(total))


def sort_kernel(in_ref, out_ref, label_ref, where_ref, sem):
    labels = in_ref[:, 2].astype(jnp.float32)[:, 0, :].astype(jnp.int32)
    label_ref[...] = labels
    copy = pltpu.make_async_copy(label_ref, where_ref, sem)
    copy.start()
    copy.wait()

    def one(i, carry):
        for slot in range(2):
            out_ref[where_ref[i, slot]] = in_ref[i, slot]
        return carry

    lax.fori_loop(0, in_ref.shape[0], one, 0)


def sort_pieces(spread):
    count, _, piece, lanes = spread.shape
    return pl.pallas_call(
        sort_kernel,
        in_specs=[pl.BlockSpec(memory_space=pltpu.VMEM)],
        out_specs=pl.BlockSpec(memory_space=pltpu.VMEM),
        out_shape=jax.ShapeDtypeStruct((2 * count, piece, lanes), spread.dtype),
        scratch_shapes=[
            pltpu.VMEM((count, lanes), jnp.int32),
            pltpu.SMEM((count, lanes), jnp.int32),
            pltpu.SemaphoreType.DMA,
        ],
        compiler_params=pltpu.CompilerParams(vmem_limit_bytes=8 << 20),
        name="sort_pieces",
    )(spread)


def blank(shape, dtype):
    return pl.pallas_call(
        lambda out_ref: None,
        out_specs=pl.BlockSpec(memory_space=pl.ANY),
        out_shape=jax.ShapeDtypeStruct(shape, dtype),
        name="blank",
    )()


def attend_kernel(heads, a_ref, b_ref, k_ref, v_ref, n0_ref, n1_ref, turn_ref, out_ref):
    length = length_of(pl.program_id(0), n0_ref, n1_ref)
    total = a_ref.shape[1]
    keys, values = k_ref[0], v_ref[0]
    row = lax.broadcasted_iota(jnp.int32, (total, total), 0)
    column = lax.broadcasted_iota(jnp.int32, (total, total), 1)
    allowed = (row >= column) & (column < length)
    for h in range(heads):
        columns = slice(h * HD, (h + 1) * HD)
        query = turned(a_ref[0, :, columns] + b_ref[0, :, columns], turn_ref)
        scores = lax.dot_general(
            query, keys, (((1,), (1,)), ((), ())), preferred_element_type=jnp.float32
        ) * (1.0 / math.sqrt(HD))
        scores = jnp.where(allowed, scores, -jnp.inf)
        peak = jnp.max(scores, axis=-1, keepdims=True)
        expo = jnp.exp(scores - peak)
        share = 1.0 / jnp.sum(expo, axis=-1, keepdims=True)
        weights = (expo * share).astype(jnp.bfloat16)
        out_ref[:, columns] = jnp.dot(
            weights, values, preferred_element_type=jnp.float32
        ).astype(jnp.bfloat16)


def turns(total):
    steps = np.arange(HD // 2, dtype=np.float32) * np.float32(2.0 / HD)
    freq = np.power(np.float32(ROPE_BASE), -steps)
    angle = np.arange(total, dtype=np.float32)[:, None] * freq[None, :]
    return np.concatenate([np.cos(angle), np.sin(angle)], axis=1).astype(np.float32)


def attend(kept, other, keys, values, first, second):
    _, total, wide = kept.shape
    rows = pl.BlockSpec((1, total, wide), lambda s: (s, 0, 0))
    note = pl.BlockSpec((16, HD), lambda s: (0, first.shape[1] // HD - 1))
    each = pl.BlockSpec((1, total, HD), lambda s: (s, 0, 0))
    return pl.pallas_call(
        functools.partial(attend_kernel, wide // HD),
        grid=(2,),
        in_specs=[rows, rows, each, each, note, note, pl.BlockSpec((total, HD), lambda s: (0, 0))],
        out_specs=pl.BlockSpec((total, wide), lambda s: (s, 0)),
        out_shape=jax.ShapeDtypeStruct((2 * total, wide), jnp.bfloat16),
        compiler_params=pltpu.CompilerParams(vmem_limit_bytes=24 << 20),
        name="attend",
    )(kept, other, keys, values, first, second, turns(total))


def output_kernel(shift_ref, a0, a1, a2, a3, a4, near_ref, far_ref, out_ref, line_ref):
    half = a0.shape[0] // 2

    @pl.when(pl.program_id(0) == 0)
    def _():
        for d, start, rows in ((0, 0, a0), (1, 0, a1), (2, 0, a2), (2, half, a3), (3, 0, a4)):
            place = (d + shift_ref[0]) % X
            line_ref[place, start : start + rows.shape[0], :] = rows[...]

    group = a0.shape[1]
    total = 0.0
    for place in range(X):
        ref = near_ref if place < X // 2 else far_ref
        start = place % (X // 2) * group
        total += lax.dot_general(
            line_ref[place],
            ref[:, start : start + group],
            (((1,), (1,)), ((), ())),
            preferred_element_type=jnp.float32,
        )
    out_ref[...] = total.astype(out_ref.dtype)


def project_out(mine, after, across, before, near, far, shift, pieces=4):
    total, group = mine.shape
    columns = near.shape[0]
    whole = part = pl.BlockSpec(memory_space=pltpu.VMEM)
    weights = pl.BlockSpec((columns // pieces, near.shape[1]), lambda i, w: (i, 0))
    return pl.pallas_call(
        output_kernel,
        grid_spec=pltpu.PrefetchScalarGridSpec(
            num_scalar_prefetch=1,
            grid=(pieces,),
            in_specs=[whole, whole, part, part, whole, weights, weights],
            out_specs=pl.BlockSpec((total, columns // pieces), lambda i, w: (0, i)),
            scratch_shapes=[pltpu.VMEM((X, total, group), mine.dtype)],
        ),
        out_shape=jax.ShapeDtypeStruct((total, columns), jnp.bfloat16),
        compiler_params=pltpu.CompilerParams(vmem_limit_bytes=24 << 20),
        name="project_out",
    )(shift.reshape(1), mine, after, *across, before, near, far)


def on_device(normed, q_weight, kv_weight, o_weight, lengths, destinations):
    ring = lax.axis_size("z")
    move = mover(ring)
    x, z, t = lax.axis_index("x"), lax.axis_index("z"), lax.axis_index("tensor")
    odd = x % 2 == 1

    total, width = normed.shape[1:]
    rows = q_weight.shape[0]
    group = q_weight.shape[1] // 2
    plus = lambda x, z, t: (x + 1, z, t)
    minus = lambda x, z, t: (x - 1, z, t)
    up = lambda x, z, t: (x, z + 1, t)
    down = lambda x, z, t: (x, z - 1, t)
    swap = lambda x, z, t: (x, z, 1 - t)

    note = jnp.repeat(jnp.stack([lengths, destinations], axis=1), HD // 2, axis=1)
    note = jnp.broadcast_to(note.astype(jnp.bfloat16), (rows, HD))

    def columns(b):
        q = lax.dynamic_slice(q_weight, (0, b * group), (rows, group))
        kv = lax.dynamic_slice(kv_weight, (0, 0, b * HD), (rows, 2, HD))
        return jnp.concatenate([q, kv[:, 0], kv[:, 1], note], axis=1)

    part0 = move(columns(x % 2), lambda x, z, t: (2 * t + x % 2, z, x // 2))
    part1 = move(columns((x + 1) % 2), lambda x, z, t: (2 * t + (x + 1) % 2, z, x // 2))
    first = jnp.where(odd, part1, part0)
    second = jnp.where(odd, part0, part1)
    wide = group + 2 * HD

    block = jnp.concatenate([first[:, :wide], second[:, :wide], o_weight.T], axis=1)
    full_in = blank((ring, rows, 2 * wide), block.dtype)
    full_out = blank((ring, rows, block.shape[1] - 2 * wide), block.dtype)

    def place(full, block, index, row=0):
        at = (index % ring, row, 0)
        return (
            lax.dynamic_update_slice(full[0], block[None, :, : 2 * wide], at),
            lax.dynamic_update_slice(full[1], block[None, :, 2 * wide :], at),
        )

    full = full_in, full_out
    rising = falling = block
    last = ring // 2
    for k in range(1, last):
        placed = place(full, rising, z - k + 1)
        if k > 1:
            placed = place(placed, falling, z + k - 1)
        rising = move(rising, up)
        falling = move(falling, down)
        rising, falling, full = lax.optimization_barrier((rising, falling, placed))
        if k == START:
            half = width // 2
            rising, normed = lax.optimization_barrier((rising, normed))
            own = lax.dynamic_slice(normed[0], (0, t * half), (total, half))
            before = move(own, plus)
            after = move(own, minus)
            across0 = move(before[: total // 2], plus)
            across1 = move(after[total // 2 :], minus)
    full = place(place(full, rising, z - last + 1), falling, z + last - 1)
    cut = rows // 2
    full = place(full, move(rising[:cut], up), z - last)
    full_in, full_out = place(full, move(falling[cut:], down), z + last, cut)

    o_half = full_out.reshape(ring * rows, -1)
    o_other = move(o_half, swap)

    states = blank((X, total, half), own.dtype)
    for piece, d, row in (
        (own, 0, 0),
        (before, -1, 0),
        (after, 1, 0),
        (across0, 2, 0),
        (across1, 2, total // 2),
    ):
        states = lax.dynamic_update_slice(states, piece[None], ((x + d) % X, row, 0))
    pieces = group // (2 * HD)
    other = move(project_in(states, full_in, 1 - t, pieces, 1), swap)
    kept = project_in(states, full_in, t, pieces, 1)
    keys, values, sent = make_cache(kept, other, first, second, ring)
    spread = lax.all_to_all(
        sent.reshape(-1, *sent.shape[2:]), ("z", "tensor"), 0, 0, tiled=True
    )
    other = move(project_in(states, full_in, 1 - t, 0, pieces), swap)
    kept = project_in(states, full_in, t, 0, pieces)

    mixed = attend(kept, other, keys, values, first, second)
    from_before = move(mixed, plus)
    from_after = move(mixed, minus)
    across = move(from_before[:total], plus), move(from_after[total:], minus)
    out = project_out(
        mixed, from_after, across, from_before, o_half, o_other, (x - 2 * t) % X
    )
    out0 = lax.dynamic_slice(out, (x % 2 * total, 0), (total, out.shape[1]))
    out1 = lax.dynamic_slice(out, ((x + 1) % 2 * total, 0), (total, out.shape[1]))
    home0 = move(out0, lambda x, z, t: (2 * t + x % 2, z, x // 2))
    home1 = move(out1, lambda x, z, t: (2 * t + (x + 1) % 2, z, x // 2))
    projected = jnp.concatenate(
        [jnp.where(odd, home1, home0), jnp.where(odd, home0, home1)], axis=1
    )

    sorted_pieces = sort_pieces(spread)
    arrived = lax.all_to_all(sorted_pieces, ("x", "z"), 0, 0, tiled=True)
    routed = arrived.reshape(X, 2, total // 2, HD).transpose(1, 0, 2, 3)
    return (projected[None], routed[None])


def solution(mesh):
    parts, count, cores = mesh.devices.shape
    torus = Mesh(
        mesh.devices.reshape(parts, X, count // X, cores), ("parts", "x", "z", "tensor")
    )
    placed = (
        P(("parts", "x", "z"), None, None),
        P(("x", "z"), "tensor"),
        P(("x", "z"), None, "tensor"),
        P("tensor", ("x", "z")),
        P(("parts", "x", "z")),
        P(("parts", "x", "z")),
    )

    return jax.shard_map(
        on_device,
        mesh=torus,
        in_specs=placed,
        out_specs=(
            P(("parts", "x", "z"), None, "tensor"),
            P(("parts", "x", "z"), None, None, "tensor", None),
        ),
        check_vma=False,
    )
```

```python
import functools
import math

import jax
import jax.numpy as jnp
import numpy as np
from jax import lax
from jax.experimental import pallas as pl
from jax.experimental.pallas import tpu as pltpu
from jax.sharding import Mesh
from jax.sharding import PartitionSpec as P

HD = 128
ROPE_BASE = 500000.0
START = 2
LABEL = 8
X = 4


def mover(ring):
    def move(array, where):
        pairs = []
        for x in range(X):
            for z in range(ring):
                for t in range(2):
                    a, b, c = where(x, z, t)
                    target = ((a % X) * ring + b % ring) * 2 + c
                    pairs.append(((x * ring + z) * 2 + t, target))
        return lax.ppermute(array, ("x", "z", "tensor"), pairs)

    return move


def project_kernel(pair_ref, x_ref, w_ref, out_ref):
    slots, total, depth = x_ref.shape
    weights = w_ref[...].reshape(depth, w_ref.shape[2])
    product = jnp.dot(
        x_ref[...].reshape(slots * total, depth), weights, preferred_element_type=jnp.float32
    ).reshape(slots, total, -1)
    width = weights.shape[1]
    columns = pl.ds(pl.multiple_of(pl.program_id(1) * width, width), width)

    @pl.when(pl.program_id(0) == 0)
    def _():
        out_ref[:, :, columns] = product

    @pl.when(pl.program_id(0) > 0)
    def _():
        out_ref[:, :, columns] += product


def project_in(states, weights, pair, first, pieces):
    _, total, half = states.shape
    ring, rows, both = weights.shape
    width = 2 * HD
    jump = both // 2 // width
    return pl.pallas_call(
        project_kernel,
        grid_spec=pltpu.PrefetchScalarGridSpec(
            num_scalar_prefetch=1,
            grid=(2, pieces),
            in_specs=[
                pl.BlockSpec((2, total, half // 2), lambda b, n, p: (p[0], 0, b)),
                pl.BlockSpec((ring, rows, width), lambda b, n, p: (0, 0, b * jump + first + n)),
            ],
            out_specs=pl.BlockSpec((2, total, pieces * width), lambda b, n, p: (0, 0, 0)),
        ),
        out_shape=jax.ShapeDtypeStruct((2, total, pieces * width), jnp.float32),
        compiler_params=pltpu.CompilerParams(vmem_limit_bytes=24 << 20),
        name="project_in",
    )(pair.reshape(1), states, weights)


def turned(values, turn_ref):
    cosine = jnp.concatenate([turn_ref[:, : HD // 2]] * 2, axis=1)
    sine = jnp.concatenate([-turn_ref[:, HD // 2 :], turn_ref[:, HD // 2 :]], axis=1)
    swapped = pltpu.roll(values, HD // 2, 1)
    return (values * cosine + swapped * sine).astype(jnp.bfloat16)


def length_of(slot, first_ref, second_ref):
    note = jnp.where(slot == 0, first_ref[:1, :1], second_ref[:1, :1])
    return note.astype(jnp.float32).astype(jnp.int32)


def cache_kernel(a_ref, b_ref, n0_ref, n1_ref, turn_ref, keys_ref, values_ref, sent_ref):
    slot = pl.program_id(0)
    length = length_of(slot, n0_ref, n1_ref)
    total = a_ref.shape[1]
    sums = a_ref[0] + b_ref[0]
    keys = turned(sums[:, :HD], turn_ref)
    values = sums[:, HD:].astype(jnp.bfloat16)
    keys_ref[0] = keys
    values_ref[0] = values
    live = lax.broadcasted_iota(jnp.int32, (total, HD), 0) < length
    zero = jnp.zeros((), jnp.bfloat16)
    ring, cores, piece, _ = sent_ref.shape
    piece = (piece - LABEL) // 2
    count = ring // 2
    at = pl.ds(pl.multiple_of(slot * piece, piece), piece)
    for index, array in enumerate((keys, values)):
        kept = jnp.where(live, array, zero).reshape(cores, count, piece, HD)
        for core in range(cores):
            sent_ref[index * count : (index + 1) * count, core, at] = kept[core]

    @pl.when(slot == 0)
    def _():
        lane = lax.broadcasted_iota(jnp.int32, (LABEL, HD), 1)
        half = HD // 2
        label = jnp.where(lane == 0, n0_ref[:1, half : half + 1], n1_ref[:1, half : half + 1])
        label = jnp.broadcast_to(label, (ring, cores, LABEL, HD))
        sent_ref[:, :, 2 * piece :] = label


def make_cache(kept, other, first, second, ring):
    _, total, wide = kept.shape
    rows = pl.BlockSpec((1, total, wide), lambda s: (s, 0, 0))
    note = pl.BlockSpec((16, HD), lambda s: (0, first.shape[1] // HD - 1))
    each = pl.BlockSpec((1, total, HD), lambda s: (s, 0, 0))
    sent = (ring, 2, 2 * (total // ring) + LABEL, HD)
    return pl.pallas_call(
        cache_kernel,
        grid=(2,),
        in_specs=[rows, rows, note, note, pl.BlockSpec((total, HD), lambda s: (0, 0))],
        out_specs=[each, each, pl.BlockSpec(sent, lambda s: (0, 0, 0, 0))],
        out_shape=[
            jax.ShapeDtypeStruct((2, total, HD), jnp.bfloat16),
            jax.ShapeDtypeStruct((2, total, HD), jnp.bfloat16),
            jax.ShapeDtypeStruct(sent, jnp.bfloat16),
        ],
        compiler_params=pltpu.CompilerParams(vmem_limit_bytes=24 << 20),
        name="make_cache",
    )(kept, other, first, second, turns(total))


def sort_kernel(in_ref, out_ref, label_ref, where_ref, sem):
    piece = out_ref.shape[1]
    labels = in_ref[:, 2 * piece :].astype(jnp.float32)[:, 0, :].astype(jnp.int32)
    label_ref[...] = labels
    copy = pltpu.make_async_copy(label_ref, where_ref, sem)
    copy.start()
    copy.wait()

    def one(i, carry):
        for slot in range(2):
            out_ref[where_ref[i, slot]] = in_ref[i, slot * piece : (slot + 1) * piece]
        return carry

    lax.fori_loop(0, in_ref.shape[0], one, 0)


def sort_pieces(spread):
    count, piece, lanes = spread.shape
    piece = (piece - LABEL) // 2
    return pl.pallas_call(
        sort_kernel,
        in_specs=[pl.BlockSpec(memory_space=pltpu.VMEM)],
        out_specs=pl.BlockSpec(memory_space=pltpu.VMEM),
        out_shape=jax.ShapeDtypeStruct((2 * count, piece, lanes), spread.dtype),
        scratch_shapes=[
            pltpu.VMEM((count, lanes), jnp.int32),
            pltpu.SMEM((count, lanes), jnp.int32),
            pltpu.SemaphoreType.DMA,
        ],
        compiler_params=pltpu.CompilerParams(vmem_limit_bytes=8 << 20),
        name="sort_pieces",
    )(spread)


def blank(shape, dtype):
    return pl.pallas_call(
        lambda out_ref: None,
        out_specs=pl.BlockSpec(memory_space=pl.ANY),
        out_shape=jax.ShapeDtypeStruct(shape, dtype),
        name="blank",
    )()


def attend_kernel(heads, a_ref, b_ref, k_ref, v_ref, n0_ref, n1_ref, turn_ref, out_ref):
    length = length_of(pl.program_id(0), n0_ref, n1_ref)
    total = a_ref.shape[1]
    keys, values = k_ref[0], v_ref[0]
    row = lax.broadcasted_iota(jnp.int32, (total, total), 0)
    column = lax.broadcasted_iota(jnp.int32, (total, total), 1)
    allowed = (row >= column) & (column < length)
    for h in range(heads):
        columns = slice(h * HD, (h + 1) * HD)
        query = turned(a_ref[0, :, columns] + b_ref[0, :, columns], turn_ref)
        scores = lax.dot_general(
            query, keys, (((1,), (1,)), ((), ())), preferred_element_type=jnp.float32
        ) * (1.0 / math.sqrt(HD))
        scores = jnp.where(allowed, scores, -jnp.inf)
        peak = jnp.max(scores, axis=-1, keepdims=True)
        expo = jnp.exp(scores - peak)
        share = 1.0 / jnp.sum(expo, axis=-1, keepdims=True)
        weights = (expo * share).astype(jnp.bfloat16)
        out_ref[:, columns] = jnp.dot(
            weights, values, preferred_element_type=jnp.float32
        ).astype(jnp.bfloat16)


def turns(total):
    steps = np.arange(HD // 2, dtype=np.float32) * np.float32(2.0 / HD)
    freq = np.power(np.float32(ROPE_BASE), -steps)
    angle = np.arange(total, dtype=np.float32)[:, None] * freq[None, :]
    return np.concatenate([np.cos(angle), np.sin(angle)], axis=1).astype(np.float32)


def attend(kept, other, keys, values, first, second):
    _, total, wide = kept.shape
    rows = pl.BlockSpec((1, total, wide), lambda s: (s, 0, 0))
    note = pl.BlockSpec((16, HD), lambda s: (0, first.shape[1] // HD - 1))
    each = pl.BlockSpec((1, total, HD), lambda s: (s, 0, 0))
    return pl.pallas_call(
        functools.partial(attend_kernel, wide // HD),
        grid=(2,),
        in_specs=[rows, rows, each, each, note, note, pl.BlockSpec((total, HD), lambda s: (0, 0))],
        out_specs=pl.BlockSpec((total, wide), lambda s: (s, 0)),
        out_shape=jax.ShapeDtypeStruct((2 * total, wide), jnp.bfloat16),
        compiler_params=pltpu.CompilerParams(vmem_limit_bytes=24 << 20),
        name="attend",
    )(kept, other, keys, values, first, second, turns(total))


def output_kernel(shift_ref, a0, a1, a2, a3, a4, near_ref, far_ref, out_ref, line_ref):
    half = a0.shape[0] // 2

    @pl.when(pl.program_id(0) == 0)
    def _():
        for d, start, rows in ((0, 0, a0), (1, 0, a1), (2, 0, a2), (2, half, a3), (3, 0, a4)):
            place = (d + shift_ref[0]) % X
            line_ref[place, start : start + rows.shape[0], :] = rows[...]

    group = a0.shape[1]
    total = 0.0
    for place in range(X):
        ref = near_ref if place < X // 2 else far_ref
        start = place % (X // 2) * group
        total += lax.dot_general(
            line_ref[place],
            ref[:, start : start + group],
            (((1,), (1,)), ((), ())),
            preferred_element_type=jnp.float32,
        )
    out_ref[...] = total.astype(out_ref.dtype)


def project_out(mine, after, across, before, near, far, shift, pieces=4):
    total, group = mine.shape
    columns = near.shape[0]
    whole = part = pl.BlockSpec(memory_space=pltpu.VMEM)
    weights = pl.BlockSpec((columns // pieces, near.shape[1]), lambda i, w: (i, 0))
    return pl.pallas_call(
        output_kernel,
        grid_spec=pltpu.PrefetchScalarGridSpec(
            num_scalar_prefetch=1,
            grid=(pieces,),
            in_specs=[whole, whole, part, part, whole, weights, weights],
            out_specs=pl.BlockSpec((total, columns // pieces), lambda i, w: (0, i)),
            scratch_shapes=[pltpu.VMEM((X, total, group), mine.dtype)],
        ),
        out_shape=jax.ShapeDtypeStruct((total, columns), jnp.bfloat16),
        compiler_params=pltpu.CompilerParams(vmem_limit_bytes=24 << 20),
        name="project_out",
    )(shift.reshape(1), mine, after, *across, before, near, far)


def on_device(normed, q_weight, kv_weight, o_weight, lengths, destinations):
    ring = lax.axis_size("z")
    move = mover(ring)
    x, z, t = lax.axis_index("x"), lax.axis_index("z"), lax.axis_index("tensor")
    odd = x % 2 == 1

    total, width = normed.shape[1:]
    rows = q_weight.shape[0]
    group = q_weight.shape[1] // 2
    plus = lambda x, z, t: (x + 1, z, t)
    minus = lambda x, z, t: (x - 1, z, t)
    up = lambda x, z, t: (x, z + 1, t)
    down = lambda x, z, t: (x, z - 1, t)
    swap = lambda x, z, t: (x, z, 1 - t)

    note = jnp.repeat(jnp.stack([lengths, destinations], axis=1), HD // 2, axis=1)
    note = jnp.broadcast_to(note.astype(jnp.bfloat16), (rows, HD))

    def columns(b):
        q = lax.dynamic_slice(q_weight, (0, b * group), (rows, group))
        kv = lax.dynamic_slice(kv_weight, (0, 0, b * HD), (rows, 2, HD))
        return jnp.concatenate([q, kv[:, 0], kv[:, 1], note], axis=1)

    part0 = move(columns(x % 2), lambda x, z, t: (2 * t + x % 2, z, x // 2))
    part1 = move(columns((x + 1) % 2), lambda x, z, t: (2 * t + (x + 1) % 2, z, x // 2))
    first = jnp.where(odd, part1, part0)
    second = jnp.where(odd, part0, part1)
    wide = group + 2 * HD

    block = jnp.concatenate([first[:, :wide], second[:, :wide], o_weight.T], axis=1)
    full_in = blank((ring, rows, 2 * wide), block.dtype)
    full_out = blank((ring, rows, block.shape[1] - 2 * wide), block.dtype)

    def place(full, block, index, row=0):
        at = (index % ring, row, 0)
        return (
            lax.dynamic_update_slice(full[0], block[None, :, : 2 * wide], at),
            lax.dynamic_update_slice(full[1], block[None, :, 2 * wide :], at),
        )

    full = full_in, full_out
    rising = falling = block
    last = ring // 2
    for k in range(1, last):
        placed = place(full, rising, z - k + 1)
        if k > 1:
            placed = place(placed, falling, z + k - 1)
        rising = move(rising, up)
        falling = move(falling, down)
        rising, falling, full = lax.optimization_barrier((rising, falling, placed))
        if k == START:
            half = width // 2
            rising, normed = lax.optimization_barrier((rising, normed))
            own = lax.dynamic_slice(normed[0], (0, t * half), (total, half))
            before = move(own, plus)
            after = move(own, minus)
            across0 = move(before[: total // 2], plus)
            across1 = move(after[total // 2 :], minus)
    full = place(place(full, rising, z - last + 1), falling, z + last - 1)
    cut = rows // 2
    full = place(full, move(rising[:cut], up), z - last)
    full_in, full_out = place(full, move(falling[cut:], down), z + last, cut)

    o_half = full_out.reshape(ring * rows, -1)
    o_other = move(o_half, swap)

    states = blank((X, total, half), own.dtype)
    for piece, d, row in (
        (own, 0, 0),
        (before, -1, 0),
        (after, 1, 0),
        (across0, 2, 0),
        (across1, 2, total // 2),
    ):
        states = lax.dynamic_update_slice(states, piece[None], ((x + d) % X, row, 0))
    pieces = group // (2 * HD)
    other = move(project_in(states, full_in, 1 - t, pieces, 1), swap)
    kept = project_in(states, full_in, t, pieces, 1)
    keys, values, sent = make_cache(kept, other, first, second, ring)
    spread = lax.all_to_all(
        sent.reshape(-1, *sent.shape[2:]), ("z", "tensor"), 0, 0, tiled=True
    )
    other = project_in(states, full_in, 1 - t, 0, pieces)
    other = move(other, swap)
    kept = project_in(states, full_in, t, 0, pieces)

    mixed = attend(kept, other, keys, values, first, second)
    from_before = move(mixed, plus)
    from_after = move(mixed, minus)
    across = move(from_before[:total], plus), move(from_after[total:], minus)
    out = project_out(
        mixed, from_after, across, from_before, o_half, o_other, (x - 2 * t) % X
    )
    out0 = lax.dynamic_slice(out, (x % 2 * total, 0), (total, out.shape[1]))
    out1 = lax.dynamic_slice(out, ((x + 1) % 2 * total, 0), (total, out.shape[1]))
    home0 = move(out0, lambda x, z, t: (2 * t + x % 2, z, x // 2))
    home1 = move(out1, lambda x, z, t: (2 * t + (x + 1) % 2, z, x // 2))
    projected = jnp.concatenate(
        [jnp.where(odd, home1, home0), jnp.where(odd, home0, home1)], axis=1
    )

    sorted_pieces = sort_pieces(spread)
    arrived = lax.all_to_all(sorted_pieces, ("x", "z"), 0, 0, tiled=True)
    routed = arrived.reshape(X, 2, total // 2, HD).transpose(1, 0, 2, 3)
    return (projected[None], routed[None])


def solution(mesh):
    parts, count, cores = mesh.devices.shape
    torus = Mesh(
        mesh.devices.reshape(parts, X, count // X, cores), ("parts", "x", "z", "tensor")
    )
    placed = (
        P(("parts", "x", "z"), None, None),
        P(("x", "z"), "tensor"),
        P(("x", "z"), None, "tensor"),
        P("tensor", ("x", "z")),
        P(("parts", "x", "z")),
        P(("parts", "x", "z")),
    )

    return jax.shard_map(
        on_device,
        mesh=torus,
        in_specs=placed,
        out_specs=(
            P(("parts", "x", "z"), None, "tensor"),
            P(("parts", "x", "z"), None, None, "tensor", None),
        ),
        check_vma=False,
    )
```

```python
import functools
import math

import jax
import jax.numpy as jnp
import numpy as np
from jax import lax
from jax.experimental import pallas as pl
from jax.experimental.pallas import tpu as pltpu
from jax.sharding import Mesh
from jax.sharding import PartitionSpec as P

HD = 128
ROPE_BASE = 500000.0
START = 2
LABEL = 8
X = 4


def mover(ring):
    def move(array, where):
        pairs = []
        for x in range(X):
            for z in range(ring):
                for t in range(2):
                    a, b, c = where(x, z, t)
                    target = ((a % X) * ring + b % ring) * 2 + c
                    pairs.append(((x * ring + z) * 2 + t, target))
        return lax.ppermute(array, ("x", "z", "tensor"), pairs)

    return move


def project_kernel(pair_ref, x_ref, w_ref, out_ref):
    slots, total, depth = x_ref.shape
    weights = w_ref[...].reshape(depth, w_ref.shape[2])
    product = jnp.dot(
        x_ref[...].reshape(slots * total, depth), weights, preferred_element_type=jnp.float32
    ).reshape(slots, total, -1)
    width = weights.shape[1]
    columns = pl.ds(pl.multiple_of(pl.program_id(1) * width, width), width)

    @pl.when(pl.program_id(0) == 0)
    def _():
        out_ref[:, :, columns] = product

    @pl.when(pl.program_id(0) > 0)
    def _():
        out_ref[:, :, columns] += product


def project_in(states, weights, pair, first, pieces):
    _, total, half = states.shape
    ring, rows, both = weights.shape
    width = 2 * HD
    jump = both // 2 // width
    return pl.pallas_call(
        project_kernel,
        grid_spec=pltpu.PrefetchScalarGridSpec(
            num_scalar_prefetch=1,
            grid=(2, pieces),
            in_specs=[
                pl.BlockSpec((2, total, half // 2), lambda b, n, p: (p[0], 0, b)),
                pl.BlockSpec((ring, rows, width), lambda b, n, p: (0, 0, b * jump + first + n)),
            ],
            out_specs=pl.BlockSpec((2, total, pieces * width), lambda b, n, p: (0, 0, 0)),
        ),
        out_shape=jax.ShapeDtypeStruct((2, total, pieces * width), jnp.float32),
        compiler_params=pltpu.CompilerParams(vmem_limit_bytes=24 << 20),
        name="project_in",
    )(pair.reshape(1), states, weights)


def turned(values, turn_ref):
    cosine = jnp.concatenate([turn_ref[:, : HD // 2]] * 2, axis=1)
    sine = jnp.concatenate([-turn_ref[:, HD // 2 :], turn_ref[:, HD // 2 :]], axis=1)
    swapped = pltpu.roll(values, HD // 2, 1)
    return (values * cosine + swapped * sine).astype(jnp.bfloat16)


def length_of(slot, first_ref, second_ref):
    note = jnp.where(slot == 0, first_ref[:1, :1], second_ref[:1, :1])
    return note.astype(jnp.float32).astype(jnp.int32)


def cache_kernel(a_ref, b_ref, n0_ref, n1_ref, turn_ref, keys_ref, values_ref, sent_ref):
    slot = pl.program_id(0)
    length = length_of(slot, n0_ref, n1_ref)
    total = a_ref.shape[1]
    sums = a_ref[0] + b_ref[0]
    keys = turned(sums[:, :HD], turn_ref)
    values = sums[:, HD:].astype(jnp.bfloat16)
    keys_ref[0] = keys
    values_ref[0] = values
    live = lax.broadcasted_iota(jnp.int32, (total, HD), 0) < length
    zero = jnp.zeros((), jnp.bfloat16)
    ring, cores, piece, _ = sent_ref.shape
    piece = (piece - LABEL) // 2
    count = ring // 2
    at = pl.ds(pl.multiple_of(slot * piece, piece), piece)
    for index, array in enumerate((keys, values)):
        kept = jnp.where(live, array, zero).reshape(cores, count, piece, HD)
        for core in range(cores):
            sent_ref[index * count : (index + 1) * count, core, at] = kept[core]

    @pl.when(slot == 0)
    def _():
        lane = lax.broadcasted_iota(jnp.int32, (LABEL, HD), 1)
        half = HD // 2
        label = jnp.where(lane == 0, n0_ref[:1, half : half + 1], n1_ref[:1, half : half + 1])
        label = jnp.broadcast_to(label, (ring, cores, LABEL, HD))
        sent_ref[:, :, 2 * piece :] = label


def make_cache(kept, other, first, second, ring):
    _, total, wide = kept.shape
    rows = pl.BlockSpec((1, total, wide), lambda s: (s, 0, 0))
    note = pl.BlockSpec((16, HD), lambda s: (0, first.shape[1] // HD - 1))
    each = pl.BlockSpec((1, total, HD), lambda s: (s, 0, 0))
    sent = (ring, 2, 2 * (total // ring) + LABEL, HD)
    return pl.pallas_call(
        cache_kernel,
        grid=(2,),
        in_specs=[rows, rows, note, note, pl.BlockSpec((total, HD), lambda s: (0, 0))],
        out_specs=[each, each, pl.BlockSpec(sent, lambda s: (0, 0, 0, 0))],
        out_shape=[
            pltpu.HBM((2, total, HD), jnp.bfloat16),
            pltpu.HBM((2, total, HD), jnp.bfloat16),
            pltpu.HBM(sent, jnp.bfloat16),
        ],
        compiler_params=pltpu.CompilerParams(vmem_limit_bytes=24 << 20),
        name="make_cache",
    )(kept, other, first, second, turns(total))


def sort_kernel(in_ref, out_ref, label_ref, where_ref, sem):
    piece = out_ref.shape[1]
    labels = in_ref[:, 2 * piece :].astype(jnp.float32)[:, 0, :].astype(jnp.int32)
    label_ref[...] = labels
    copy = pltpu.make_async_copy(label_ref, where_ref, sem)
    copy.start()
    copy.wait()

    def one(i, carry):
        for slot in range(2):
            out_ref[where_ref[i, slot]] = in_ref[i, slot * piece : (slot + 1) * piece]
        return carry

    lax.fori_loop(0, in_ref.shape[0], one, 0)


def sort_pieces(spread):
    count, piece, lanes = spread.shape
    piece = (piece - LABEL) // 2
    return pl.pallas_call(
        sort_kernel,
        in_specs=[pl.BlockSpec(memory_space=pltpu.VMEM)],
        out_specs=pl.BlockSpec(memory_space=pltpu.VMEM),
        out_shape=jax.ShapeDtypeStruct((2 * count, piece, lanes), spread.dtype),
        scratch_shapes=[
            pltpu.VMEM((count, lanes), jnp.int32),
            pltpu.SMEM((count, lanes), jnp.int32),
            pltpu.SemaphoreType.DMA,
        ],
        compiler_params=pltpu.CompilerParams(vmem_limit_bytes=8 << 20),
        name="sort_pieces",
    )(spread)


def blank(shape, dtype):
    return pl.pallas_call(
        lambda out_ref: None,
        out_specs=pl.BlockSpec(memory_space=pl.ANY),
        out_shape=jax.ShapeDtypeStruct(shape, dtype),
        name="blank",
    )()


def attend_kernel(heads, a_ref, b_ref, k_ref, v_ref, n0_ref, n1_ref, turn_ref, out_ref):
    length = length_of(pl.program_id(0), n0_ref, n1_ref)
    total = a_ref.shape[1]
    keys, values = k_ref[0], v_ref[0]
    row = lax.broadcasted_iota(jnp.int32, (total, total), 0)
    column = lax.broadcasted_iota(jnp.int32, (total, total), 1)
    allowed = (row >= column) & (column < length)
    for h in range(heads):
        columns = slice(h * HD, (h + 1) * HD)
        query = turned(a_ref[0, :, columns] + b_ref[0, :, columns], turn_ref)
        scores = lax.dot_general(
            query, keys, (((1,), (1,)), ((), ())), preferred_element_type=jnp.float32
        ) * (1.0 / math.sqrt(HD))
        scores = jnp.where(allowed, scores, -jnp.inf)
        peak = jnp.max(scores, axis=-1, keepdims=True)
        expo = jnp.exp(scores - peak)
        share = 1.0 / jnp.sum(expo, axis=-1, keepdims=True)
        weights = (expo * share).astype(jnp.bfloat16)
        out_ref[:, columns] = jnp.dot(
            weights, values, preferred_element_type=jnp.float32
        ).astype(jnp.bfloat16)


def turns(total):
    steps = np.arange(HD // 2, dtype=np.float32) * np.float32(2.0 / HD)
    freq = np.power(np.float32(ROPE_BASE), -steps)
    angle = np.arange(total, dtype=np.float32)[:, None] * freq[None, :]
    return np.concatenate([np.cos(angle), np.sin(angle)], axis=1).astype(np.float32)


def attend(kept, other, keys, values, first, second):
    _, total, wide = kept.shape
    rows = pl.BlockSpec((1, total, wide), lambda s: (s, 0, 0))
    note = pl.BlockSpec((16, HD), lambda s: (0, first.shape[1] // HD - 1))
    each = pl.BlockSpec((1, total, HD), lambda s: (s, 0, 0))
    return pl.pallas_call(
        functools.partial(attend_kernel, wide // HD),
        grid=(2,),
        in_specs=[rows, rows, each, each, note, note, pl.BlockSpec((total, HD), lambda s: (0, 0))],
        out_specs=pl.BlockSpec((total, wide), lambda s: (s, 0)),
        out_shape=jax.ShapeDtypeStruct((2 * total, wide), jnp.bfloat16),
        compiler_params=pltpu.CompilerParams(vmem_limit_bytes=24 << 20),
        name="attend",
    )(kept, other, keys, values, first, second, turns(total))


def output_kernel(shift_ref, a0, a1, a2, a3, a4, near_ref, far_ref, out_ref, line_ref, sems):
    half = a2.shape[0]

    @pl.when(pl.program_id(0) == 0)
    def _():
        place = (2 + shift_ref[0]) % X
        copies = [
            pltpu.make_async_copy(rows, line_ref.at[place, pl.ds(k * half, half)], sems.at[k])
            for k, rows in enumerate((a2, a3))
        ]
        for copy in copies:
            copy.start()
        for d, rows in ((0, a0), (1, a1), (3, a4)):
            line_ref[(d + shift_ref[0]) % X] = rows[...]
        for copy in copies:
            copy.wait()

    group = a0.shape[1]
    total = 0.0
    for place in range(X):
        ref = near_ref if place < X // 2 else far_ref
        start = place % (X // 2) * group
        total += lax.dot_general(
            line_ref[place],
            ref[:, start : start + group],
            (((1,), (1,)), ((), ())),
            preferred_element_type=jnp.float32,
        )
    out_ref[...] = total.astype(out_ref.dtype)


def project_out(mine, after, across, before, near, far, shift, pieces=4):
    total, group = mine.shape
    columns = near.shape[0]
    whole = pl.BlockSpec(memory_space=pltpu.VMEM)
    part = pl.BlockSpec(memory_space=pl.ANY)
    weights = pl.BlockSpec((columns // pieces, near.shape[1]), lambda i, w: (i, 0))
    return pl.pallas_call(
        output_kernel,
        grid_spec=pltpu.PrefetchScalarGridSpec(
            num_scalar_prefetch=1,
            grid=(pieces,),
            in_specs=[whole, whole, part, part, whole, weights, weights],
            out_specs=pl.BlockSpec((total, columns // pieces), lambda i, w: (0, i)),
            scratch_shapes=[
                pltpu.VMEM((X, total, group), mine.dtype),
                pltpu.SemaphoreType.DMA((2,)),
            ],
        ),
        out_shape=jax.ShapeDtypeStruct((total, columns), jnp.bfloat16),
        compiler_params=pltpu.CompilerParams(vmem_limit_bytes=24 << 20),
        name="project_out",
    )(shift.reshape(1), mine, after, *across, before, near, far)


def on_device(normed, q_weight, kv_weight, o_weight, lengths, destinations):
    ring = lax.axis_size("z")
    move = mover(ring)
    x, z, t = lax.axis_index("x"), lax.axis_index("z"), lax.axis_index("tensor")
    odd = x % 2 == 1

    total, width = normed.shape[1:]
    rows = q_weight.shape[0]
    group = q_weight.shape[1] // 2
    plus = lambda x, z, t: (x + 1, z, t)
    minus = lambda x, z, t: (x - 1, z, t)
    up = lambda x, z, t: (x, z + 1, t)
    down = lambda x, z, t: (x, z - 1, t)
    swap = lambda x, z, t: (x, z, 1 - t)

    note = jnp.repeat(jnp.stack([lengths, destinations], axis=1), HD // 2, axis=1)
    note = jnp.broadcast_to(note.astype(jnp.bfloat16), (rows, HD))

    def columns(b):
        q = lax.dynamic_slice(q_weight, (0, b * group), (rows, group))
        kv = lax.dynamic_slice(kv_weight, (0, 0, b * HD), (rows, 2, HD))
        return jnp.concatenate([q, kv[:, 0], kv[:, 1], note], axis=1)

    part0 = move(columns(x % 2), lambda x, z, t: (2 * t + x % 2, z, x // 2))
    part1 = move(columns((x + 1) % 2), lambda x, z, t: (2 * t + (x + 1) % 2, z, x // 2))
    first = jnp.where(odd, part1, part0)
    second = jnp.where(odd, part0, part1)
    wide = group + 2 * HD

    block = jnp.concatenate([first[:, :wide], second[:, :wide], o_weight.T], axis=1)
    full_in = blank((ring, rows, 2 * wide), block.dtype)
    full_out = blank((ring, rows, block.shape[1] - 2 * wide), block.dtype)

    def place(full, block, index, row=0):
        at = (index % ring, row, 0)
        return (
            lax.dynamic_update_slice(full[0], block[None, :, : 2 * wide], at),
            lax.dynamic_update_slice(full[1], block[None, :, 2 * wide :], at),
        )

    full = full_in, full_out
    rising = falling = block
    last = ring // 2
    for k in range(1, last):
        placed = place(full, rising, z - k + 1)
        if k > 1:
            placed = place(placed, falling, z + k - 1)
        rising = move(rising, up)
        falling = move(falling, down)
        rising, falling, full = lax.optimization_barrier((rising, falling, placed))
        if k == START:
            half = width // 2
            rising, normed = lax.optimization_barrier((rising, normed))
            own = lax.dynamic_slice(normed[0], (0, t * half), (total, half))
            before = move(own, plus)
            after = move(own, minus)
            across0 = move(before[: total // 2], plus)
            across1 = move(after[total // 2 :], minus)
    full = place(place(full, rising, z - last + 1), falling, z + last - 1)
    cut = rows // 2
    full = place(full, move(rising[:cut], up), z - last)
    full_in, full_out = place(full, move(falling[cut:], down), z + last, cut)

    o_half = full_out.reshape(ring * rows, -1)
    o_other = move(o_half, swap)

    states = blank((X, total, half), own.dtype)
    for piece, d, row in (
        (own, 0, 0),
        (before, -1, 0),
        (after, 1, 0),
        (across0, 2, 0),
        (across1, 2, total // 2),
    ):
        states = lax.dynamic_update_slice(states, piece[None], ((x + d) % X, row, 0))
    pieces = group // (2 * HD)
    other = move(project_in(states, full_in, 1 - t, pieces, 1), swap)
    kept = project_in(states, full_in, t, pieces, 1)
    keys, values, sent = make_cache(kept, other, first, second, ring)
    spread = lax.all_to_all(sent.reshape(-1, *sent.shape[2:]), ("z", "tensor"), 0, 0, tiled=True)
    other = project_in(states, full_in, 1 - t, 0, pieces)
    other = move(other, swap)
    kept = project_in(states, full_in, t, 0, pieces)

    mixed = attend(kept, other, keys, values, first, second)
    from_before = move(mixed, plus)
    from_after = move(mixed, minus)
    across = move(from_before[:total], plus), move(from_after[total:], minus)
    out = project_out(
        mixed, from_after, across, from_before, o_half, o_other, (x - 2 * t) % X
    )
    out0 = lax.dynamic_slice(out, (x % 2 * total, 0), (total, out.shape[1]))
    out1 = lax.dynamic_slice(out, ((x + 1) % 2 * total, 0), (total, out.shape[1]))
    home0 = move(out0, lambda x, z, t: (2 * t + x % 2, z, x // 2))
    home1 = move(out1, lambda x, z, t: (2 * t + (x + 1) % 2, z, x // 2))
    projected = jnp.concatenate(
        [jnp.where(odd, home1, home0), jnp.where(odd, home0, home1)], axis=1
    )

    sorted_pieces = sort_pieces(spread)
    arrived = lax.all_to_all(sorted_pieces, ("x", "z"), 0, 0, tiled=True)
    routed = arrived.reshape(X, 2, total // 2, HD).transpose(1, 0, 2, 3)
    return (projected[None], routed[None])


def solution(mesh):
    parts, count, cores = mesh.devices.shape
    torus = Mesh(
        mesh.devices.reshape(parts, X, count // X, cores), ("parts", "x", "z", "tensor")
    )
    placed = (
        P(("parts", "x", "z"), None, None),
        P(("x", "z"), "tensor"),
        P(("x", "z"), None, "tensor"),
        P("tensor", ("x", "z")),
        P(("parts", "x", "z")),
        P(("parts", "x", "z")),
    )

    return jax.shard_map(
        on_device,
        mesh=torus,
        in_specs=placed,
        out_specs=(
            P(("parts", "x", "z"), None, "tensor"),
            P(("parts", "x", "z"), None, None, "tensor", None),
        ),
        check_vma=False,
    )
```

```python
import functools
import math

import jax
import jax.numpy as jnp
import numpy as np
from jax import lax
from jax.experimental import pallas as pl
from jax.experimental.pallas import tpu as pltpu
from jax.sharding import Mesh
from jax.sharding import PartitionSpec as P

HD = 128
ROPE_BASE = 500000.0
START = 2
LABEL = 8
X = 4


def mover(ring):
    def move(array, where):
        pairs = []
        for x in range(X):
            for z in range(ring):
                for t in range(2):
                    a, b, c = where(x, z, t)
                    target = ((a % X) * ring + b % ring) * 2 + c
                    pairs.append(((x * ring + z) * 2 + t, target))
        return lax.ppermute(array, ("x", "z", "tensor"), pairs)

    return move


def project_kernel(pair_ref, x_ref, w_ref, out_ref):
    slots, total, depth = x_ref.shape
    weights = w_ref[...].reshape(depth, w_ref.shape[2])
    product = jnp.dot(
        x_ref[...].reshape(slots * total, depth), weights, preferred_element_type=jnp.float32
    ).reshape(slots, total, -1)
    width = weights.shape[1]
    columns = pl.ds(pl.multiple_of(pl.program_id(1) * width, width), width)

    @pl.when(pl.program_id(0) == 0)
    def _():
        out_ref[:, :, columns] = product

    @pl.when(pl.program_id(0) > 0)
    def _():
        out_ref[:, :, columns] += product


def project_in(states, weights, pair, first, pieces):
    _, total, half = states.shape
    ring, rows, both = weights.shape
    width = 2 * HD
    jump = both // 2 // width
    return pl.pallas_call(
        project_kernel,
        grid_spec=pltpu.PrefetchScalarGridSpec(
            num_scalar_prefetch=1,
            grid=(2, pieces),
            in_specs=[
                pl.BlockSpec((2, total, half // 2), lambda b, n, p: (p[0], 0, b)),
                pl.BlockSpec((ring, rows, width), lambda b, n, p: (0, 0, b * jump + first + n)),
            ],
            out_specs=pl.BlockSpec((2, total, pieces * width), lambda b, n, p: (0, 0, 0)),
        ),
        out_shape=jax.ShapeDtypeStruct((2, total, pieces * width), jnp.float32),
        compiler_params=pltpu.CompilerParams(vmem_limit_bytes=24 << 20),
        name="project_in",
    )(pair.reshape(1), states, weights)


def turned(values, turn_ref):
    cosine = jnp.concatenate([turn_ref[:, : HD // 2]] * 2, axis=1)
    sine = jnp.concatenate([-turn_ref[:, HD // 2 :], turn_ref[:, HD // 2 :]], axis=1)
    swapped = pltpu.roll(values, HD // 2, 1)
    return (values * cosine + swapped * sine).astype(jnp.bfloat16)


def length_of(slot, first_ref, second_ref):
    note = jnp.where(slot == 0, first_ref[:1, :1], second_ref[:1, :1])
    return note.astype(jnp.float32).astype(jnp.int32)


def cache_kernel(a_ref, b_ref, n0_ref, n1_ref, turn_ref, keys_ref, values_ref, sent_ref):
    slot = pl.program_id(0)
    length = length_of(slot, n0_ref, n1_ref)
    total = a_ref.shape[1]
    sums = a_ref[0] + b_ref[0]
    keys = turned(sums[:, :HD], turn_ref)
    values = sums[:, HD:].astype(jnp.bfloat16)
    keys_ref[0] = keys
    values_ref[0] = values
    live = lax.broadcasted_iota(jnp.int32, (total, HD), 0) < length
    zero = jnp.zeros((), jnp.bfloat16)
    ring, cores, piece, _ = sent_ref.shape
    piece = (piece - LABEL) // 2
    count = ring // 2
    at = pl.ds(pl.multiple_of(slot * piece, piece), piece)
    for index, array in enumerate((keys, values)):
        kept = jnp.where(live, array, zero).reshape(cores, count, piece, HD)
        for core in range(cores):
            sent_ref[index * count : (index + 1) * count, core, at] = kept[core]

    @pl.when(slot == 0)
    def _():
        lane = lax.broadcasted_iota(jnp.int32, (LABEL, HD), 1)
        half = HD // 2
        label = jnp.where(lane == 0, n0_ref[:1, half : half + 1], n1_ref[:1, half : half + 1])
        label = jnp.broadcast_to(label, (ring, cores, LABEL, HD))
        sent_ref[:, :, 2 * piece :] = label


def make_cache(kept, other, first, second, ring):
    _, total, wide = kept.shape
    rows = pl.BlockSpec((1, total, wide), lambda s: (s, 0, 0))
    note = pl.BlockSpec((16, HD), lambda s: (0, first.shape[1] // HD - 1))
    each = pl.BlockSpec((1, total, HD), lambda s: (s, 0, 0))
    sent = (ring, 2, 2 * (total // ring) + LABEL, HD)
    return pl.pallas_call(
        cache_kernel,
        grid=(2,),
        in_specs=[rows, rows, note, note, pl.BlockSpec((total, HD), lambda s: (0, 0))],
        out_specs=[each, each, pl.BlockSpec(sent, lambda s: (0, 0, 0, 0))],
        out_shape=[
            pltpu.HBM((2, total, HD), jnp.bfloat16),
            pltpu.HBM((2, total, HD), jnp.bfloat16),
            pltpu.HBM(sent, jnp.bfloat16),
        ],
        compiler_params=pltpu.CompilerParams(vmem_limit_bytes=24 << 20),
        name="make_cache",
    )(kept, other, first, second, turns(total))


def sort_kernel(in_ref, out_ref, label_ref, where_ref, sem):
    piece = out_ref.shape[1]
    labels = in_ref[:, 2 * piece :].astype(jnp.float32)[:, 0, :].astype(jnp.int32)
    label_ref[...] = labels
    copy = pltpu.make_async_copy(label_ref, where_ref, sem)
    copy.start()
    copy.wait()

    def one(i, carry):
        for slot in range(2):
            out_ref[where_ref[i, slot]] = in_ref[i, slot * piece : (slot + 1) * piece]
        return carry

    lax.fori_loop(0, in_ref.shape[0], one, 0)


def sort_pieces(spread):
    count, piece, lanes = spread.shape
    piece = (piece - LABEL) // 2
    return pl.pallas_call(
        sort_kernel,
        in_specs=[pl.BlockSpec(memory_space=pltpu.VMEM)],
        out_specs=pl.BlockSpec(memory_space=pltpu.VMEM),
        out_shape=jax.ShapeDtypeStruct((2 * count, piece, lanes), spread.dtype),
        scratch_shapes=[
            pltpu.VMEM((count, lanes), jnp.int32),
            pltpu.SMEM((count, lanes), jnp.int32),
            pltpu.SemaphoreType.DMA,
        ],
        compiler_params=pltpu.CompilerParams(vmem_limit_bytes=8 << 20),
        name="sort_pieces",
    )(spread)


def blank(shape, dtype):
    return pl.pallas_call(
        lambda out_ref: None,
        out_specs=pl.BlockSpec(memory_space=pl.ANY),
        out_shape=jax.ShapeDtypeStruct(shape, dtype),
        name="blank",
    )()


def attend_kernel(heads, a_ref, b_ref, k_ref, v_ref, n0_ref, n1_ref, turn_ref, out_ref):
    length = length_of(pl.program_id(0), n0_ref, n1_ref)
    total = a_ref.shape[1]
    keys, values = k_ref[0], v_ref[0]
    row = lax.broadcasted_iota(jnp.int32, (total, total), 0)
    column = lax.broadcasted_iota(jnp.int32, (total, total), 1)
    allowed = (row >= column) & (column < length)
    for h in range(heads):
        columns = slice(h * HD, (h + 1) * HD)
        query = turned(a_ref[0, :, columns] + b_ref[0, :, columns], turn_ref)
        scores = lax.dot_general(
            query, keys, (((1,), (1,)), ((), ())), preferred_element_type=jnp.float32
        ) * (1.0 / math.sqrt(HD))
        scores = jnp.where(allowed, scores, -jnp.inf)
        peak = jnp.max(scores, axis=-1, keepdims=True)
        expo = jnp.exp(scores - peak)
        share = 1.0 / jnp.sum(expo, axis=-1, keepdims=True)
        weights = (expo * share).astype(jnp.bfloat16)
        out_ref[:, columns] = jnp.dot(
            weights, values, preferred_element_type=jnp.float32
        ).astype(jnp.bfloat16)


def turns(total):
    steps = np.arange(HD // 2, dtype=np.float32) * np.float32(2.0 / HD)
    freq = np.power(np.float32(ROPE_BASE), -steps)
    angle = np.arange(total, dtype=np.float32)[:, None] * freq[None, :]
    return np.concatenate([np.cos(angle), np.sin(angle)], axis=1).astype(np.float32)


def attend(kept, other, keys, values, first, second):
    _, total, wide = kept.shape
    rows = pl.BlockSpec((1, total, wide), lambda s: (s, 0, 0))
    note = pl.BlockSpec((16, HD), lambda s: (0, first.shape[1] // HD - 1))
    each = pl.BlockSpec((1, total, HD), lambda s: (s, 0, 0))
    return pl.pallas_call(
        functools.partial(attend_kernel, wide // HD),
        grid=(2,),
        in_specs=[rows, rows, each, each, note, note, pl.BlockSpec((total, HD), lambda s: (0, 0))],
        out_specs=pl.BlockSpec((total, wide), lambda s: (s, 0)),
        out_shape=jax.ShapeDtypeStruct((2 * total, wide), jnp.bfloat16),
        compiler_params=pltpu.CompilerParams(vmem_limit_bytes=24 << 20),
        name="attend",
    )(kept, other, keys, values, first, second, turns(total))


def output_kernel(shift_ref, a0, a1, a2, a3, near_ref, far_ref, out_ref, line_ref, sem):

    @pl.when(pl.program_id(0) == 0)
    def _():
        facing = line_ref.at[(2 + shift_ref[0]) % X]
        copy = pltpu.make_async_copy(a2, facing, sem)
        copy.start()
        for d, rows in ((0, a0), (1, a1), (3, a3)):
            line_ref[(d + shift_ref[0]) % X] = rows[...]
        copy.wait()

    group = a0.shape[1]
    total = 0.0
    for place in range(X):
        ref = near_ref if place < X // 2 else far_ref
        start = place % (X // 2) * group
        total += lax.dot_general(
            line_ref[place],
            ref[:, start : start + group],
            (((1,), (1,)), ((), ())),
            preferred_element_type=jnp.float32,
        )
    out_ref[...] = total.astype(out_ref.dtype)


def project_out(mine, after, facing, before, near, far, shift, pieces=4):
    total, group = mine.shape
    columns = near.shape[0]
    whole = pl.BlockSpec(memory_space=pltpu.VMEM)
    part = pl.BlockSpec(memory_space=pl.ANY)
    weights = pl.BlockSpec((columns // pieces, near.shape[1]), lambda i, w: (i, 0))
    return pl.pallas_call(
        output_kernel,
        grid_spec=pltpu.PrefetchScalarGridSpec(
            num_scalar_prefetch=1,
            grid=(pieces,),
            in_specs=[whole, whole, part, whole, weights, weights],
            out_specs=pl.BlockSpec((total, columns // pieces), lambda i, w: (0, i)),
            scratch_shapes=[
                pltpu.VMEM((X, total, group), mine.dtype),
                pltpu.SemaphoreType.DMA,
            ],
        ),
        out_shape=jax.ShapeDtypeStruct((total, columns), jnp.bfloat16),
        compiler_params=pltpu.CompilerParams(vmem_limit_bytes=24 << 20),
        name="project_out",
    )(shift.reshape(1), mine, after, facing, before, near, far)


def on_device(normed, q_weight, kv_weight, o_weight, lengths, destinations):
    ring = lax.axis_size("z")
    move = mover(ring)
    x, z, t = lax.axis_index("x"), lax.axis_index("z"), lax.axis_index("tensor")
    odd = x % 2 == 1

    total, width = normed.shape[1:]
    rows = q_weight.shape[0]
    group = q_weight.shape[1] // 2
    plus = lambda x, z, t: (x + 1, z, t)
    minus = lambda x, z, t: (x - 1, z, t)
    up = lambda x, z, t: (x, z + 1, t)
    down = lambda x, z, t: (x, z - 1, t)
    swap = lambda x, z, t: (x, z, 1 - t)

    note = jnp.repeat(jnp.stack([lengths, destinations], axis=1), HD // 2, axis=1)
    note = jnp.broadcast_to(note.astype(jnp.bfloat16), (rows, HD))

    def columns(b):
        q = lax.dynamic_slice(q_weight, (0, b * group), (rows, group))
        kv = lax.dynamic_slice(kv_weight, (0, 0, b * HD), (rows, 2, HD))
        return jnp.concatenate([q, kv[:, 0], kv[:, 1], note], axis=1)

    part0 = move(columns(x % 2), lambda x, z, t: (2 * t + x % 2, z, x // 2))
    part1 = move(columns((x + 1) % 2), lambda x, z, t: (2 * t + (x + 1) % 2, z, x // 2))
    first = jnp.where(odd, part1, part0)
    second = jnp.where(odd, part0, part1)
    wide = group + 2 * HD

    block = jnp.concatenate([first[:, :wide], second[:, :wide], o_weight.T], axis=1)
    full_in = blank((ring, rows, 2 * wide), block.dtype)
    full_out = blank((ring, rows, block.shape[1] - 2 * wide), block.dtype)

    def place(full, block, index, row=0):
        at = (index % ring, row, 0)
        return (
            lax.dynamic_update_slice(full[0], block[None, :, : 2 * wide], at),
            lax.dynamic_update_slice(full[1], block[None, :, 2 * wide :], at),
        )

    full = full_in, full_out
    rising = falling = block
    last = ring // 2
    for k in range(1, last):
        placed = place(full, rising, z - k + 1)
        if k > 1:
            placed = place(placed, falling, z + k - 1)
        rising = move(rising, up)
        falling = move(falling, down)
        rising, falling, full = lax.optimization_barrier((rising, falling, placed))
        if k == START - 1:
            half = width // 2
            block, normed = lax.optimization_barrier((block, normed))
            own = lax.dynamic_slice(normed[0], (0, t * half), (total, half))
        if k == START:
            rising, own = lax.optimization_barrier((rising, own))
            before = move(own, plus)
            after = move(own, minus)
            across0 = move(before[: total // 2], plus)
            across1 = move(after[total // 2 :], minus)
    full = place(place(full, rising, z - last + 1), falling, z + last - 1)
    cut = rows // 2
    full = place(full, move(rising[:cut], up), z - last)
    full_in, full_out = place(full, move(falling[cut:], down), z + last, cut)

    o_half = full_out.reshape(ring * rows, -1)
    o_other = move(o_half, swap)

    states = blank((X, total, half), own.dtype)
    for piece, d, row in (
        (own, 0, 0),
        (before, -1, 0),
        (after, 1, 0),
        (across0, 2, 0),
        (across1, 2, total // 2),
    ):
        states = lax.dynamic_update_slice(states, piece[None], ((x + d) % X, row, 0))
    pieces = group // (2 * HD)
    other = move(project_in(states, full_in, 1 - t, pieces, 1), swap)
    kept = project_in(states, full_in, t, pieces, 1)
    keys, values, sent = make_cache(kept, other, first, second, ring)
    spread = lax.all_to_all(
        sent.reshape(-1, *sent.shape[2:]), ("z", "tensor"), 0, 0, tiled=True
    )
    other = project_in(states, full_in, 1 - t, 0, pieces)
    other = move(other, swap)
    kept = project_in(states, full_in, t, 0, pieces)

    mixed = attend(kept, other, keys, values, first, second)
    from_before = move(mixed, plus)
    from_after = move(mixed, minus)
    facing = move(mixed, lambda x, z, t: (x + 2, z, t))
    out = project_out(
        mixed, from_after, facing, from_before, o_half, o_other, (x - 2 * t) % X
    )
    out0 = lax.dynamic_slice(out, (x % 2 * total, 0), (total, out.shape[1]))
    out1 = lax.dynamic_slice(out, ((x + 1) % 2 * total, 0), (total, out.shape[1]))
    home0 = move(out0, lambda x, z, t: (2 * t + x % 2, z, x // 2))
    home1 = move(out1, lambda x, z, t: (2 * t + (x + 1) % 2, z, x // 2))
    projected = jnp.concatenate(
        [jnp.where(odd, home1, home0), jnp.where(odd, home0, home1)], axis=1
    )

    sorted_pieces = sort_pieces(spread)
    arrived = lax.all_to_all(sorted_pieces, ("x", "z"), 0, 0, tiled=True)
    routed = arrived.reshape(X, 2, total // 2, HD).transpose(1, 0, 2, 3)
    return (projected[None], routed[None])


def solution(mesh):
    parts, count, cores = mesh.devices.shape
    torus = Mesh(
        mesh.devices.reshape(parts, X, count // X, cores), ("parts", "x", "z", "tensor")
    )
    placed = (
        P(("parts", "x", "z"), None, None),
        P(("x", "z"), "tensor"),
        P(("x", "z"), None, "tensor"),
        P("tensor", ("x", "z")),
        P(("parts", "x", "z")),
        P(("parts", "x", "z")),
    )

    return jax.shard_map(
        on_device,
        mesh=torus,
        in_specs=placed,
        out_specs=(
            P(("parts", "x", "z"), None, "tensor"),
            P(("parts", "x", "z"), None, None, "tensor", None),
        ),
        check_vma=False,
    )
```
